32 devices in a mesh: row: 4 (over z), col: 2 (over y), layer: 4 (over x, core).
Axes of the slice: x: 2, y: 2, z: 4, core: 2. Of those that a mesh axis runs over, the one named last changes fastest.
Arguments:
- tokens: bfloat16 [1280, 6144], P('row', 'layer'), may hold values from -6 to 6
- expert_ids: int32 [1280, 2], replicated, may hold values from 0 to 7, all different within a row; in each aligned block of 1280 rows (0 to 1279, 1280 to 2559, ...) at most 640 rows name the same one
- w_gate: bfloat16 [2, 6144, 8192], P(None, 'layer', ('row', 'col')), may hold values from -0.078125 to 0.078125
- w_up: bfloat16 [2, 6144, 8192], P(None, 'layer', ('row', 'col')), may hold values from -0.078125 to 0.078125
Outputs:
- hidden: bfloat16 [2, 640, 8192], P(None, ('col', 'layer'), 'row')
The draws below stay inside these ranges and needn't reach their ends.
Inputs may be any that keep to these rules, and one draw needn't show every extreme that they name: `expert_ids`: each token names 2 different experts. No expert is named by more than 640 tokens, a bound that some block reaches.
All inputs are finite; a program needn't handle non-finite values.
Results may differ from the reference program's by a relative error of at most 0.0012.
Values may be sent and summed in bfloat16 or wider, within the bound.
A program may use at most 128 MiB of HBM per device.

```python
import math
import jax
import jax.numpy as jnp
import numpy as np

D = 6144
EXPERTS = 8
TOP = 2
FF = 8192
EXP_FLIGHT = 2
SLOTS_DEV = 80
CAP = 640
TOKENS = 1280
N_COL = 2
N_LAYER = 4


def block_scale(stream_key, extent, shards, low, top_value):
    def one(axis_at, shards_of):
        heights = jax.random.uniform(jax.random.fold_in(jax.random.fold_in(stream_key, 6), axis_at), (shards_of,), jnp.float32, low / len(shards), top_value / len(shards))
        return jnp.repeat(jnp.exp(heights), extent[axis_at] // shards_of).reshape((-1,) + (1,) * (len(extent) - axis_at - 1))

    factor_of = one(*shards[0])
    for cut in shards[1:]:
        factor_of = factor_of * one(*cut)
    return factor_of


def deal_out(rng, own, number, rows, number_of, top, most, slope):
    order = jax.random.permutation(rng, number_of)
    heavy_load, ordinary = load_shares(number_of, rows * top, most, slope, True), load_shares(number_of, rows * top, most, slope, False)
    places = jnp.arange(number_of)

    def named(lengths, offset_by):
        used = int((lengths > 0).sum())
        fixed = max(1, used // 4)
        passed = fixed + (places - fixed + offset_by * (used - fixed)) % max(1, number_of - fixed)
        return jnp.zeros((number_of,), jnp.int32).at[order[jnp.where(places < fixed, places, passed)]].set(jnp.asarray(lengths, jnp.int32))

    lengths = jnp.where(number % 4 == 0, named(heavy_load, number // 4), named(ordinary, number - number // 4 - 1))
    mixed = jax.random.permutation(jax.random.fold_in(own, 3), number_of)
    giver, receiver = mixed[0:number_of // 2 * 2:2], mixed[1:number_of // 2 * 2:2]
    room = jnp.minimum(lengths[giver] - 1, most - lengths[receiver]) // 2
    room = jnp.where((giver == order[0]) | (receiver == order[0]) | (lengths[receiver] == 0), 0, jnp.maximum(room, 0))
    passed = jax.random.randint(jax.random.fold_in(own, 4), (number_of // 2,), 0, 1 << 20) % (room + 1)
    lengths = lengths.at[giver].add(-passed).at[receiver].add(passed)
    members = jnp.searchsorted(jnp.cumsum(lengths), jnp.arange(rows * top), side="right").astype(jnp.int32)
    listing = members.reshape(top, rows).T
    listing = listing[jax.random.permutation(jax.random.fold_in(own, 1), rows)]
    offset_by = jax.random.randint(jax.random.fold_in(own, 2), (rows, 1), 0, top)
    return jnp.take_along_axis(listing, (jnp.arange(top)[None, :] + offset_by) % top, axis=1)


def load_shares(number_of, total, reach, slope, full):
    weights = [(1 << 20) // math.isqrt(standing ** slope) + 1 for standing in range(1, number_of + 1)]
    largest = reach if full else min(reach, max(-(-total // number_of), total * weights[0] // sum(weights)))
    least = 1 if total - largest >= number_of - 1 else 0
    given, surplus = [largest] + [least] * (number_of - 1), total - largest - least * (number_of - 1)
    while surplus > 0:
        candidates = [i for i in range(1, number_of) if given[i] < largest] or [i for i in range(1, number_of) if given[i] < reach]
        whole, remaining = sum([weights[i] for i in candidates]), surplus
        for i in candidates:
            addition = min(reach - given[i], max(1, remaining * weights[i] // whole), surplus)
            given[i] = given[i] + addition
            surplus = surplus - addition
    return np.array(given)


def centred(key, dims, scale, limit, shards=(), kind=jnp.bfloat16):
    loudness = block_scale(key, dims, shards, -0.22, 0.18) if shards else 1.0
    entries = jax.random.normal(key, dims, jnp.float32) * scale * loudness
    return jnp.minimum(jnp.maximum(entries, -limit), limit).astype(kind)


def setup_inputs(seed: int = 0) -> dict:
    streams_of = jax.random.split(jax.random.key(seed), 5)
    tokens = centred(streams_of[0], (TOKENS, D), 1.0, 6.0, ((0, 4), (1, 4)))
    expert_ids_keys = jax.random.split(jax.random.fold_in(streams_of[1], 1), TOKENS // TOKENS)
    expert_ids_turns = jax.random.permutation(jax.random.fold_in(streams_of[1], 3), TOKENS // TOKENS)
    expert_ids = jax.vmap(lambda own, number: deal_out(jax.random.fold_in(streams_of[1], 2), own, number, TOKENS, EXPERTS, TOP, CAP, 2))(expert_ids_keys, expert_ids_turns).reshape((TOKENS, TOP))
    w_gate = centred(streams_of[2], (EXP_FLIGHT, D, FF), D ** -0.5, 0.078125, ((1, 4), (2, 8)))
    w_up = centred(streams_of[3], (EXP_FLIGHT, D, FF), D ** -0.5, 0.078125, ((1, 4), (2, 8)))
    return {"tokens": tokens, "expert_ids": expert_ids, "w_gate": w_gate, "w_up": w_up}


def reference(tokens, expert_ids, w_gate, w_up):
    tok_count = tokens.shape[0]
    capacity = SLOTS_DEV * N_COL * N_LAYER
    expert_range = jnp.arange(EXP_FLIGHT, dtype=jnp.int32)
    member = jnp.any(expert_ids[:, :, None] == expert_range[None, None, :], axis=1).astype(jnp.int32)
    slot_rank = (jnp.cumsum(member, axis=0) - member).astype(jnp.int32)
    target = jnp.where(member > 0, slot_rank, capacity).astype(jnp.int32)
    token_range = jnp.broadcast_to(jnp.arange(tok_count, dtype=jnp.int32)[:, None], target.shape)
    slot_table = jnp.zeros((EXP_FLIGHT, capacity + 1), jnp.int32).at[expert_range[None, :], target].set(token_range)
    counts = jnp.sum(member, axis=0).astype(jnp.int32)
    live_mask = jnp.arange(capacity, dtype=jnp.int32)[None, :] < counts[:, None]
    results = []
    for expert in range(EXP_FLIGHT):
        slot_rows = jnp.where(live_mask[expert][:, None], tokens[slot_table[expert, :capacity]], jnp.zeros((), tokens.dtype))
        gate = jnp.dot(slot_rows, w_gate[expert], preferred_element_type=jnp.float32)
        up_part = jnp.dot(slot_rows, w_up[expert], preferred_element_type=jnp.float32)
        results.append((jax.nn.silu(gate) * up_part).astype(jnp.bfloat16))
    return jnp.stack(results)
```

```python
import functools

import jax
import jax.numpy as jnp
from jax import lax
from jax.experimental import pallas as pl
from jax.experimental.pallas import tpu as pltpu
from jax.sharding import PartitionSpec as P

SLOTS_DEV = 80
CHUNK = 256
PIECE = 512
MESH = pl.DeviceIdType.MESH
VMEM_LIMIT = 62 * 1024 * 1024


def slot_places(expert_ids, experts):
    expert_range = jnp.arange(experts, dtype=jnp.int32)
    member = jnp.any(expert_ids[:, :, None] == expert_range[None, None, :], axis=1).astype(
        jnp.int32
    )
    return member, jnp.cumsum(member, axis=0) - member


def plain_shards(tokens, expert_ids, w_gate, w_up):
    col_count = lax.axis_size("col")
    layer_count = lax.axis_size("layer")
    experts, _, narrow = w_gate.shape
    capacity = SLOTS_DEV * col_count * layer_count
    member, slot_rank = slot_places(expert_ids, experts)
    tok_count = expert_ids.shape[0]
    target = jnp.where(member > 0, slot_rank, capacity)
    everyone = lax.all_gather(tokens, "row", axis=0, tiled=True)
    expert_range = jnp.arange(experts, dtype=jnp.int32)
    token_range = jnp.broadcast_to(jnp.arange(tok_count, dtype=jnp.int32)[:, None], target.shape)
    slot_table = (
        jnp.zeros((experts, capacity + 1), jnp.int32)
        .at[expert_range[None, :], target]
        .set(token_range)
    )[:, :capacity]
    live = jnp.arange(capacity, dtype=jnp.int32)[None, :] < jnp.sum(member, axis=0)[:, None]
    by_layer = (experts, col_count, layer_count, SLOTS_DEV)
    slot_table = slot_table.reshape(by_layer).swapaxes(1, 2).reshape(experts, capacity)
    live = live.reshape(by_layer).swapaxes(1, 2).reshape(experts, capacity)
    slot_rows = jnp.where(live[:, :, None], everyone[slot_table], jnp.zeros((), tokens.dtype))
    totals = jnp.stack(
        [
            jnp.einsum("ecd,edf->ecf", slot_rows, w, preferred_element_type=jnp.float32)
            for w in (w_gate, w_up)
        ]
    )
    parts = lax.psum_scatter(totals, "layer", scatter_dimension=2, tiled=True)
    hidden = (jax.nn.silu(parts[0]) * parts[1]).astype(jnp.bfloat16)
    hidden = hidden.reshape(experts, col_count, SLOTS_DEV, narrow)
    return lax.all_to_all(hidden, "col", 1, 3, tiled=True).reshape(
        experts, SLOTS_DEV, col_count * narrow
    )


def kernel(
    n_row,
    tok_ref,
    tgt_ref,
    wg_hbm,
    wu_hbm,
    out_ref,
    gath,
    wg,
    wu,
    slots,
    keep,
    dsend,
    drecv,
    xsend,
    xrecv,
    ysend,
    yrecv,
    w_sem,
    zs_sem,
    zr_sem,
    fs_sem,
    fr_sem,
    ds_sem,
    dr_sem,
    xs_sem,
    xr_sem,
    ys_sem,
    yr_sem,
):
    experts, depth, narrow = wg.shape
    half = slots.shape[2]
    quarter = tok_ref.shape[1]
    pieces = depth // PIECE
    per_expert = narrow // CHUNK
    chunks = experts * per_expert
    row = lax.axis_index("row")
    col = lax.axis_index("col")
    layer = lax.axis_index("layer")
    core = lax.rem(layer, 2)
    place = lax.div(layer, 2)
    right, left = lax.rem(row + 1, n_row), lax.rem(row + n_row - 1, n_row)
    other_col = {"col": 1 - col}
    other_core = {"layer": layer + 1 - 2 * core}
    other_place = {"layer": lax.rem(layer + 2, 4)}

    w_copies = [
        pltpu.make_async_copy(wg_hbm, wg, w_sem.at[0]),
        pltpu.make_async_copy(wu_hbm, wu, w_sem.at[1]),
    ]
    for copy in w_copies:
        copy.start()

    barrier = pltpu.get_barrier_semaphore()
    for who in ({"row": right}, {"row": left}, other_col, other_core, other_place):
        pl.semaphore_signal(barrier, inc=1, device_id=who, device_id_type=MESH)
    pl.semaphore_wait(barrier, 5)

    def block_of(way, step):
        return lax.rem(row + n_row - step, n_row) if way == 0 else lax.rem(row + step, n_row)

    def ring(way, step, j):
        block = block_of(way, step - 1)
        mine = 2 * way + col
        cols = pl.ds(j * PIECE, PIECE)
        at = gath.at[block, mine, :, cols]
        return pltpu.make_async_remote_copy(
            src_ref=tok_ref.at[mine, :, cols] if step == 1 else at,
            dst_ref=at,
            send_sem=zs_sem.at[way, step - 1, j],
            recv_sem=zr_sem.at[way, step - 1, j],
            device_id={"row": right if way == 0 else left},
            device_id_type=MESH,
        )

    def across(way, step, j):
        at = gath.at[block_of(way, step), 2 * way + col, :, pl.ds(j * PIECE, PIECE)]
        return pltpu.make_async_remote_copy(
            src_ref=at,
            dst_ref=at,
            send_sem=fs_sem.at[way, step - 1, j],
            recv_sem=fr_sem.at[way, step - 1, j],
            device_id=other_col,
            device_id_type=MESH,
        )

    def place_rows(ref, block, way, first):
        rows = ref[pl.ds(2 * way, 2)].reshape(2 * quarter, depth)

        def body(i, carry):
            expert, side = lax.div(i, 2), lax.rem(i, 2)
            want = tgt_ref[block, way, expert]
            here = lax.broadcasted_iota(jnp.int32, (half, 2 * quarter), 0) + side * half
            pick = jnp.where(here == want, 1.0, 0.0).astype(jnp.bfloat16)
            got = jnp.dot(pick, rows, preferred_element_type=jnp.float32).astype(jnp.bfloat16)
            slots[expert, side] = got if first else slots[expert, side] + got
            return carry

        lax.fori_loop(0, 2 * experts, body, 0)

    for j in range(pieces):
        for way in range(2):
            ring(way, 1, j).start()
    place_rows(tok_ref, row, 0, True)
    place_rows(tok_ref, row, 1, False)

    def settle(step):
        for way in range(2):
            for j in range(pieces):
                across(way, step, j).wait_recv()
            block = block_of(way, step)
            place_rows(gath.at[block], block, way, False)

    for step in range(1, n_row):
        for j in range(pieces):
            for way in range(2):
                ring(way, step, j).wait_recv()
                if step + 1 < n_row:
                    ring(way, step + 1, j).start()
                across(way, step, j).start()
        if step > 1:
            settle(step - 1)
    settle(n_row - 1)

    for copy in w_copies:
        copy.wait()

    def core_copy(i):
        return pltpu.make_async_remote_copy(
            src_ref=dsend.at[i],
            dst_ref=drecv.at[i],
            send_sem=ds_sem.at[i],
            recv_sem=dr_sem.at[i],
            device_id=other_core,
            device_id_type=MESH,
        )

    def place_copy(i):
        return pltpu.make_async_remote_copy(
            src_ref=xsend.at[i],
            dst_ref=xrecv.at[i],
            send_sem=xs_sem.at[i],
            recv_sem=xr_sem.at[i],
            device_id=other_place,
            device_id_type=MESH,
        )

    def col_copy(i):
        return pltpu.make_async_remote_copy(
            src_ref=ysend.at[i],
            dst_ref=yrecv.at[i],
            send_sem=ys_sem.at[i],
            recv_sem=yr_sem.at[i],
            device_id=other_col,
            device_id_type=MESH,
        )

    def multiply(i):
        expert, part = lax.div(i, per_expert), lax.rem(i, per_expert)
        cols = pl.ds(pl.multiple_of(part * CHUNK, CHUNK), CHUNK)
        for side, into in ((1 - core, dsend), (core, keep)):
            rows = slots[expert, side]
            for which, w in enumerate((wg, wu)):
                got = jnp.dot(rows, w[expert, :, cols], preferred_element_type=jnp.float32)
                into[i, which] = got.reshape(2, 2, SLOTS_DEV, CHUNK)
        core_copy(i).start()

    def pass_on(i):
        core_copy(i).wait_recv()
        away = 1 - place
        for which in range(2):
            xsend[i, which] = keep[i, which, away] + drecv[i, which, away]
        place_copy(i).start()

    def first_loop(i, carry):
        multiply(i)

        @pl.when(i > 0)
        def _():
            pass_on(i - 1)

        return carry

    lax.fori_loop(0, chunks, first_loop, 0)
    pass_on(chunks - 1)

    def finished(i, side):
        gate, up = [
            keep[i, which, place, side] + drecv[i, which, place, side] + xrecv[i, which, side]
            for which in range(2)
        ]
        return (gate / (1.0 + jnp.exp(-gate)) * up).astype(jnp.bfloat16)

    def columns(i, of_col):
        start = of_col * narrow + lax.rem(i, per_expert) * CHUNK
        return pl.ds(pl.multiple_of(start, CHUNK), CHUNK)

    def finish(i):
        place_copy(i).wait_recv()
        ysend[i] = finished(i, 1 - col)
        out_ref[lax.div(i, per_expert), :, columns(i, col)] = finished(i, col)
        col_copy(i).start()

    def take(i):
        col_copy(i).wait_recv()
        out_ref[lax.div(i, per_expert), :, columns(i, 1 - col)] = yrecv[i]

    def second_loop(i, carry):
        finish(i)

        @pl.when(i > 0)
        def _():
            take(i - 1)

        return carry

    lax.fori_loop(0, chunks, second_loop, 0)
    take(chunks - 1)

    for step in range(1, n_row):
        for way in range(2):
            for j in range(pieces):
                ring(way, step, j).wait_send()
                across(way, step, j).wait_send()

    def last_loop(i, carry):
        core_copy(i).wait_send()
        place_copy(i).wait_send()
        col_copy(i).wait_send()
        return carry

    lax.fori_loop(0, chunks, last_loop, 0)


def vmem_plan(n_row, tokens, w_gate):
    local_rows, depth = tokens.shape
    experts, _, narrow = w_gate.shape
    capacity = SLOTS_DEV * 8
    chunks = experts * narrow // CHUNK
    bf, f32 = jnp.bfloat16, jnp.float32
    return [
        ((n_row, 4, local_rows // 4, depth), bf),
        (w_gate.shape, bf),
        (w_gate.shape, bf),
        ((experts, 2, capacity // 2, depth), bf),
        ((chunks, 2, 2, 2, SLOTS_DEV, CHUNK), f32),
        ((chunks, 2, 2, 2, SLOTS_DEV, CHUNK), f32),
        ((chunks, 2, 2, 2, SLOTS_DEV, CHUNK), f32),
        ((chunks, 2, 2, SLOTS_DEV, CHUNK), f32),
        ((chunks, 2, 2, SLOTS_DEV, CHUNK), f32),
        ((chunks, SLOTS_DEV, CHUNK), bf),
        ((chunks, SLOTS_DEV, CHUNK), bf),
    ]


def fits(n_row, n_col, n_layer, tokens, w_gate):
    local_rows, depth = tokens.shape
    narrow = w_gate.shape[2]
    if n_col != 2 or n_layer != 4 or n_row < 3:
        return False
    if local_rows % 64 or depth % PIECE or narrow % CHUNK:
        return False
    need = sum(
        functools.reduce(lambda a, b: a * b, shape) * jnp.dtype(kind).itemsize
        for shape, kind in vmem_plan(n_row, tokens, w_gate)
    )
    return need < VMEM_LIMIT - 8 * 1024 * 1024


def fused_shards(tokens, expert_ids, w_gate, w_up):
    n_row = lax.axis_size("row")
    experts, depth, narrow = w_gate.shape
    local_rows = tokens.shape[0]
    quarter = local_rows // 4
    chunks = experts * narrow // CHUNK
    pieces = depth // PIECE
    member, rank = slot_places(expert_ids, experts)
    of_col, of_layer, inner = rank // (4 * SLOTS_DEV), rank // SLOTS_DEV % 4, rank % SLOTS_DEV
    spot = ((of_layer % 2 * 2 + of_layer // 2) * 2 + of_col) * SLOTS_DEV + inner
    target = jnp.where(member > 0, spot, -1)
    target = target.reshape(n_row, 2, 1, 2 * quarter, experts).transpose(0, 1, 4, 2, 3)
    dma = pltpu.SemaphoreType.DMA
    ring_sems = dma((2, n_row - 1, pieces))
    return pl.pallas_call(
        functools.partial(kernel, n_row),
        out_shape=jax.ShapeDtypeStruct((experts, SLOTS_DEV, 2 * narrow), jnp.bfloat16),
        in_specs=[
            pl.BlockSpec(memory_space=pltpu.VMEM),
            pl.BlockSpec(memory_space=pltpu.VMEM),
            pl.BlockSpec(memory_space=pl.ANY),
            pl.BlockSpec(memory_space=pl.ANY),
        ],
        out_specs=pl.BlockSpec(memory_space=pltpu.VMEM),
        scratch_shapes=[
            pltpu.VMEM(shape, kind) for shape, kind in vmem_plan(n_row, tokens, w_gate)
        ]
        + [dma((2,))]
        + [ring_sems] * 4
        + [dma((chunks,))] * 6,
        compiler_params=pltpu.CompilerParams(
            collective_id=0, has_side_effects=True, vmem_limit_bytes=VMEM_LIMIT
        ),
    )(tokens.reshape(4, quarter, depth), target, w_gate, w_up)


def solution(mesh):
    def shards(tokens, expert_ids, w_gate, w_up):
        sizes = [mesh.shape[axis] for axis in ("row", "col", "layer")]
        plan = fused_shards if fits(*sizes, tokens, w_gate) else plain_shards
        return plan(tokens, expert_ids, w_gate, w_up)

    in_specs = (
        P("row", "layer"),
        P(),
        P(None, "layer", ("row", "col")),
        P(None, "layer", ("row", "col")),
    )
    out_specs = P(None, ("col", "layer"), "row")
    return jax.shard_map(shards, mesh=mesh, in_specs=in_specs, out_specs=out_specs, check_vma=False)
```

```python
import functools

import jax
import jax.numpy as jnp
from jax import lax
from jax.experimental import pallas as pl
from jax.experimental.pallas import tpu as pltpu
from jax.sharding import PartitionSpec as P

SLOTS_DEV = 80
CHUNK = 256
PIECE = 512
STEPS = 32767.0
TINY = 1e-30
MESH = pl.DeviceIdType.MESH
VMEM_LIMIT = 62 * 1024 * 1024


def slot_places(expert_ids, experts):
    expert_range = jnp.arange(experts, dtype=jnp.int32)
    member = jnp.any(expert_ids[:, :, None] == expert_range[None, None, :], axis=1).astype(
        jnp.int32
    )
    return member, jnp.cumsum(member, axis=0) - member


def plain_shards(tokens, expert_ids, w_gate, w_up):
    col_count = lax.axis_size("col")
    layer_count = lax.axis_size("layer")
    experts, _, narrow = w_gate.shape
    capacity = SLOTS_DEV * col_count * layer_count
    member, slot_rank = slot_places(expert_ids, experts)
    tok_count = expert_ids.shape[0]
    target = jnp.where(member > 0, slot_rank, capacity)
    everyone = lax.all_gather(tokens, "row", axis=0, tiled=True)
    expert_range = jnp.arange(experts, dtype=jnp.int32)
    token_range = jnp.broadcast_to(jnp.arange(tok_count, dtype=jnp.int32)[:, None], target.shape)
    slot_table = (
        jnp.zeros((experts, capacity + 1), jnp.int32)
        .at[expert_range[None, :], target]
        .set(token_range)
    )[:, :capacity]
    live = jnp.arange(capacity, dtype=jnp.int32)[None, :] < jnp.sum(member, axis=0)[:, None]
    by_layer = (experts, col_count, layer_count, SLOTS_DEV)
    slot_table = slot_table.reshape(by_layer).swapaxes(1, 2).reshape(experts, capacity)
    live = live.reshape(by_layer).swapaxes(1, 2).reshape(experts, capacity)
    slot_rows = jnp.where(live[:, :, None], everyone[slot_table], jnp.zeros((), tokens.dtype))
    totals = jnp.stack(
        [
            jnp.einsum("ecd,edf->ecf", slot_rows, w, preferred_element_type=jnp.float32)
            for w in (w_gate, w_up)
        ]
    )
    parts = lax.psum_scatter(totals, "layer", scatter_dimension=2, tiled=True)
    hidden = (jax.nn.silu(parts[0]) * parts[1]).astype(jnp.bfloat16)
    hidden = hidden.reshape(experts, col_count, SLOTS_DEV, narrow)
    return lax.all_to_all(hidden, "col", 1, 3, tiled=True).reshape(
        experts, SLOTS_DEV, col_count * narrow
    )


def kernel(
    n_row,
    tok_ref,
    tgt_ref,
    wg_hbm,
    wu_hbm,
    out_ref,
    gath,
    wg,
    wu,
    slots,
    keep,
    dsend,
    drecv,
    xsend,
    xrecv,
    unit_out,
    unit_in,
    ysend,
    yrecv,
    w_sem,
    zs_sem,
    zr_sem,
    fs_sem,
    fr_sem,
    ds_sem,
    dr_sem,
    xs_sem,
    xr_sem,
    us_sem,
    ur_sem,
    ys_sem,
    yr_sem,
):
    experts, depth, narrow = wg.shape
    half = slots.shape[2]
    quarter = tok_ref.shape[1]
    pieces = depth // PIECE
    per_expert = narrow // CHUNK
    chunks = experts * per_expert
    row = lax.axis_index("row")
    col = lax.axis_index("col")
    layer = lax.axis_index("layer")
    core = lax.rem(layer, 2)
    place = lax.div(layer, 2)
    right, left = lax.rem(row + 1, n_row), lax.rem(row + n_row - 1, n_row)
    other_col = {"col": 1 - col}
    other_core = {"layer": layer + 1 - 2 * core}
    other_place = {"layer": lax.rem(layer + 2, 4)}

    w_copies = [
        pltpu.make_async_copy(wg_hbm, wg, w_sem.at[0]),
        pltpu.make_async_copy(wu_hbm, wu, w_sem.at[1]),
    ]
    for copy in w_copies:
        copy.start()

    barrier = pltpu.get_barrier_semaphore()
    for who in ({"row": right}, {"row": left}, other_col, other_core, other_place):
        pl.semaphore_signal(barrier, inc=1, device_id=who, device_id_type=MESH)
    pl.semaphore_wait(barrier, 5)

    def block_of(way, step):
        return lax.rem(row + n_row - step, n_row) if way == 0 else lax.rem(row + step, n_row)

    def ring(way, step, j):
        block = block_of(way, step - 1)
        mine = 2 * way + col
        cols = pl.ds(j * PIECE, PIECE)
        at = gath.at[block, mine, :, cols]
        return pltpu.make_async_remote_copy(
            src_ref=tok_ref.at[mine, :, cols] if step == 1 else at,
            dst_ref=at,
            send_sem=zs_sem.at[way, step - 1, j],
            recv_sem=zr_sem.at[way, step - 1, j],
            device_id={"row": right if way == 0 else left},
            device_id_type=MESH,
        )

    def across(way, step, j):
        at = gath.at[block_of(way, step), 2 * way + col, :, pl.ds(j * PIECE, PIECE)]
        return pltpu.make_async_remote_copy(
            src_ref=at,
            dst_ref=at,
            send_sem=fs_sem.at[way, step - 1, j],
            recv_sem=fr_sem.at[way, step - 1, j],
            device_id=other_col,
            device_id_type=MESH,
        )

    def place_rows(ref, block, way, first):
        rows = ref[pl.ds(2 * way, 2)].reshape(2 * quarter, depth)

        def body(i, carry):
            expert, side = lax.div(i, 2), lax.rem(i, 2)
            want = tgt_ref[block, way, expert]
            here = lax.broadcasted_iota(jnp.int32, (half, 2 * quarter), 0) + side * half
            pick = jnp.where(here == want, 1.0, 0.0).astype(jnp.bfloat16)
            got = jnp.dot(pick, rows, preferred_element_type=jnp.float32).astype(jnp.bfloat16)
            slots[expert, side] = got if first else slots[expert, side] + got
            return carry

        lax.fori_loop(0, 2 * experts, body, 0)

    for j in range(pieces):
        for way in range(2):
            ring(way, 1, j).start()
    place_rows(tok_ref, row, 0, True)
    place_rows(tok_ref, row, 1, False)

    def settle(step):
        for way in range(2):
            for j in range(pieces):
                across(way, step, j).wait_recv()
            block = block_of(way, step)
            place_rows(gath.at[block], block, way, False)

    for step in range(1, n_row):
        for j in range(pieces):
            for way in range(2):
                ring(way, step, j).wait_recv()
                if step + 1 < n_row:
                    ring(way, step + 1, j).start()
                across(way, step, j).start()
        if step > 1:
            settle(step - 1)
    settle(n_row - 1)

    for copy in w_copies:
        copy.wait()

    def core_copy(i):
        return pltpu.make_async_remote_copy(
            src_ref=dsend.at[i],
            dst_ref=drecv.at[i],
            send_sem=ds_sem.at[i],
            recv_sem=dr_sem.at[i],
            device_id=other_core,
            device_id_type=MESH,
        )

    def place_copy(i):
        return pltpu.make_async_remote_copy(
            src_ref=xsend.at[i],
            dst_ref=xrecv.at[i],
            send_sem=xs_sem.at[i],
            recv_sem=xr_sem.at[i],
            device_id=other_place,
            device_id_type=MESH,
        )

    def unit_copy(i):
        return pltpu.make_async_remote_copy(
            src_ref=unit_out.at[i],
            dst_ref=unit_in.at[i],
            send_sem=us_sem.at[i],
            recv_sem=ur_sem.at[i],
            device_id=other_place,
            device_id_type=MESH,
        )

    def col_copy(i):
        return pltpu.make_async_remote_copy(
            src_ref=ysend.at[i],
            dst_ref=yrecv.at[i],
            send_sem=ys_sem.at[i],
            recv_sem=yr_sem.at[i],
            device_id=other_col,
            device_id_type=MESH,
        )

    def multiply(i):
        expert, part = lax.div(i, per_expert), lax.rem(i, per_expert)
        cols = pl.ds(pl.multiple_of(part * CHUNK, CHUNK), CHUNK)
        for side, into in ((1 - core, dsend), (core, keep)):
            rows = slots[expert, side]
            for which, w in enumerate((wg, wu)):
                got = jnp.dot(rows, w[expert, :, cols], preferred_element_type=jnp.float32)
                into[i, which] = got.reshape(2, 2, SLOTS_DEV, CHUNK)
        core_copy(i).start()

    def pass_on(i):
        core_copy(i).wait_recv()
        away = 1 - place
        for which in range(2):
            total = keep[i, which, away] + drecv[i, which, away]
            total = total.reshape(2 * SLOTS_DEV // 8, 8, CHUNK)
            top = jnp.maximum(jnp.max(jnp.abs(total), axis=0), TINY)
            unit_out[i, which] = top * (1.0 / STEPS)
            coded = jnp.round(total * (STEPS / top)[None])
            xsend[i, which] = (
                coded.reshape(2, SLOTS_DEV, CHUNK).astype(jnp.int32).astype(jnp.int16)
            )
        unit_copy(i).start()
        place_copy(i).start()

    def first_loop(i, carry):
        multiply(i)

        @pl.when(i > 0)
        def _():
            pass_on(i - 1)

        return carry

    lax.fori_loop(0, chunks, first_loop, 0)
    pass_on(chunks - 1)

    def finished(i, side):
        sums = []
        for which in range(2):
            far = xrecv[i, which, side].astype(jnp.int32).astype(jnp.float32)
            far = far.reshape(SLOTS_DEV // 8, 8, CHUNK) * unit_in[i, which][None]
            near = keep[i, which, place, side] + drecv[i, which, place, side]
            sums.append(near + far.reshape(SLOTS_DEV, CHUNK))
        gate, up = sums
        return (gate / (1.0 + jnp.exp(-gate)) * up).astype(jnp.bfloat16)

    def columns(i, of_col):
        start = of_col * narrow + lax.rem(i, per_expert) * CHUNK
        return pl.ds(pl.multiple_of(start, CHUNK), CHUNK)

    def finish(i):
        unit_copy(i).wait_recv()
        place_copy(i).wait_recv()
        ysend[i] = finished(i, 1 - col)
        out_ref[lax.div(i, per_expert), :, columns(i, col)] = finished(i, col)
        col_copy(i).start()

    def take(i):
        col_copy(i).wait_recv()
        out_ref[lax.div(i, per_expert), :, columns(i, 1 - col)] = yrecv[i]

    def second_loop(i, carry):
        finish(i)

        @pl.when(i > 0)
        def _():
            take(i - 1)

        return carry

    lax.fori_loop(0, chunks, second_loop, 0)
    take(chunks - 1)

    for step in range(1, n_row):
        for way in range(2):
            for j in range(pieces):
                ring(way, step, j).wait_send()
                across(way, step, j).wait_send()

    def last_loop(i, carry):
        core_copy(i).wait_send()
        unit_copy(i).wait_send()
        place_copy(i).wait_send()
        col_copy(i).wait_send()
        return carry

    lax.fori_loop(0, chunks, last_loop, 0)


def vmem_plan(n_row, tokens, w_gate):
    local_rows, depth = tokens.shape
    experts, _, narrow = w_gate.shape
    capacity = SLOTS_DEV * 8
    chunks = experts * narrow // CHUNK
    bf, f32 = jnp.bfloat16, jnp.float32
    return [
        ((n_row, 4, local_rows // 4, depth), bf),
        (w_gate.shape, bf),
        (w_gate.shape, bf),
        ((experts, 2, capacity // 2, depth), bf),
        ((chunks, 2, 2, 2, SLOTS_DEV, CHUNK), f32),
        ((chunks, 2, 2, 2, SLOTS_DEV, CHUNK), f32),
        ((chunks, 2, 2, 2, SLOTS_DEV, CHUNK), f32),
        ((chunks, 2, 2, SLOTS_DEV, CHUNK), jnp.int16),
        ((chunks, 2, 2, SLOTS_DEV, CHUNK), jnp.int16),
        ((chunks, 2, 8, CHUNK), f32),
        ((chunks, 2, 8, CHUNK), f32),
        ((chunks, SLOTS_DEV, CHUNK), bf),
        ((chunks, SLOTS_DEV, CHUNK), bf),
    ]


def fits(n_row, n_col, n_layer, tokens, w_gate):
    local_rows, depth = tokens.shape
    narrow = w_gate.shape[2]
    if n_col != 2 or n_layer != 4 or n_row < 3:
        return False
    if local_rows % 64 or depth % PIECE or narrow % CHUNK:
        return False
    need = sum(
        functools.reduce(lambda a, b: a * b, shape) * jnp.dtype(kind).itemsize
        for shape, kind in vmem_plan(n_row, tokens, w_gate)
    )
    return need < VMEM_LIMIT - 8 * 1024 * 1024


def fused_shards(tokens, expert_ids, w_gate, w_up):
    n_row = lax.axis_size("row")
    experts, depth, narrow = w_gate.shape
    local_rows = tokens.shape[0]
    quarter = local_rows // 4
    chunks = experts * narrow // CHUNK
    pieces = depth // PIECE
    member, rank = slot_places(expert_ids, experts)
    of_col, of_layer, inner = rank // (4 * SLOTS_DEV), rank // SLOTS_DEV % 4, rank % SLOTS_DEV
    spot = ((of_layer % 2 * 2 + of_layer // 2) * 2 + of_col) * SLOTS_DEV + inner
    target = jnp.where(member > 0, spot, -1)
    target = target.reshape(n_row, 2, 1, 2 * quarter, experts).transpose(0, 1, 4, 2, 3)
    dma = pltpu.SemaphoreType.DMA
    ring_sems = dma((2, n_row - 1, pieces))
    return pl.pallas_call(
        functools.partial(kernel, n_row),
        out_shape=jax.ShapeDtypeStruct((experts, SLOTS_DEV, 2 * narrow), jnp.bfloat16),
        in_specs=[
            pl.BlockSpec(memory_space=pltpu.VMEM),
            pl.BlockSpec(memory_space=pltpu.VMEM),
            pl.BlockSpec(memory_space=pl.ANY),
            pl.BlockSpec(memory_space=pl.ANY),
        ],
        out_specs=pl.BlockSpec(memory_space=pltpu.VMEM),
        scratch_shapes=[
            pltpu.VMEM(shape, kind) for shape, kind in vmem_plan(n_row, tokens, w_gate)
        ]
        + [dma((2,))]
        + [ring_sems] * 4
        + [dma((chunks,))] * 8,
        compiler_params=pltpu.CompilerParams(
            collective_id=0, has_side_effects=True, vmem_limit_bytes=VMEM_LIMIT
        ),
    )(tokens.reshape(4, quarter, depth), target, w_gate, w_up)


def solution(mesh):
    def shards(tokens, expert_ids, w_gate, w_up):
        sizes = [mesh.shape[axis] for axis in ("row", "col", "layer")]
        plan = fused_shards if fits(*sizes, tokens, w_gate) else plain_shards
        return plan(tokens, expert_ids, w_gate, w_up)

    in_specs = (
        P("row", "layer"),
        P(),
        P(None, "layer", ("row", "col")),
        P(None, "layer", ("row", "col")),
    )
    out_specs = P(None, ("col", "layer"), "row")
    return jax.shard_map(shards, mesh=mesh, in_specs=in_specs, out_specs=out_specs, check_vma=False)
```

```python
import functools

import jax
import jax.numpy as jnp
from jax import lax
from jax.experimental import pallas as pl
from jax.experimental.pallas import tpu as pltpu
from jax.sharding import PartitionSpec as P

SLOTS_DEV = 80
CHUNK = 256
PIECE = 256
STEPS = 32767.0
TINY = 1e-30
MESH = pl.DeviceIdType.MESH
VMEM_LIMIT = 62 * 1024 * 1024


def slot_places(expert_ids, experts):
    expert_range = jnp.arange(experts, dtype=jnp.int32)
    member = jnp.any(expert_ids[:, :, None] == expert_range[None, None, :], axis=1).astype(
        jnp.int32
    )
    return member, jnp.cumsum(member, axis=0) - member


def plain_shards(tokens, expert_ids, w_gate, w_up):
    col_count = lax.axis_size("col")
    layer_count = lax.axis_size("layer")
    experts, _, narrow = w_gate.shape
    capacity = SLOTS_DEV * col_count * layer_count
    member, slot_rank = slot_places(expert_ids, experts)
    tok_count = expert_ids.shape[0]
    target = jnp.where(member > 0, slot_rank, capacity)
    everyone = lax.all_gather(tokens, "row", axis=0, tiled=True)
    expert_range = jnp.arange(experts, dtype=jnp.int32)
    token_range = jnp.broadcast_to(jnp.arange(tok_count, dtype=jnp.int32)[:, None], target.shape)
    slot_table = (
        jnp.zeros((experts, capacity + 1), jnp.int32)
        .at[expert_range[None, :], target]
        .set(token_range)
    )[:, :capacity]
    live = jnp.arange(capacity, dtype=jnp.int32)[None, :] < jnp.sum(member, axis=0)[:, None]
    by_layer = (experts, col_count, layer_count, SLOTS_DEV)
    slot_table = slot_table.reshape(by_layer).swapaxes(1, 2).reshape(experts, capacity)
    live = live.reshape(by_layer).swapaxes(1, 2).reshape(experts, capacity)
    slot_rows = jnp.where(live[:, :, None], everyone[slot_table], jnp.zeros((), tokens.dtype))
    totals = jnp.stack(
        [
            jnp.einsum("ecd,edf->ecf", slot_rows, w, preferred_element_type=jnp.float32)
            for w in (w_gate, w_up)
        ]
    )
    parts = lax.psum_scatter(totals, "layer", scatter_dimension=2, tiled=True)
    hidden = (jax.nn.silu(parts[0]) * parts[1]).astype(jnp.bfloat16)
    hidden = hidden.reshape(experts, col_count, SLOTS_DEV, narrow)
    return lax.all_to_all(hidden, "col", 1, 3, tiled=True).reshape(
        experts, SLOTS_DEV, col_count * narrow
    )


def kernel(
    n_row,
    tok_ref,
    tgt_ref,
    wg_hbm,
    wu_hbm,
    out_ref,
    gath,
    wg,
    wu,
    slots,
    keep,
    dsend,
    drecv,
    xsend,
    xrecv,
    unit_out,
    unit_in,
    ysend,
    yrecv,
    w_sem,
    zs_sem,
    zr_sem,
    fs_sem,
    fr_sem,
    ds_sem,
    dr_sem,
    xs_sem,
    xr_sem,
    us_sem,
    ur_sem,
    ys_sem,
    yr_sem,
):
    experts, depth, narrow = wg.shape
    half = slots.shape[2]
    quarter = tok_ref.shape[1]
    pieces = depth // PIECE
    per_expert = narrow // CHUNK
    chunks = experts * per_expert
    row = lax.axis_index("row")
    col = lax.axis_index("col")
    layer = lax.axis_index("layer")
    core = lax.rem(layer, 2)
    place = lax.div(layer, 2)
    right, left = lax.rem(row + 1, n_row), lax.rem(row + n_row - 1, n_row)
    other_col = {"col": 1 - col}
    other_core = {"layer": layer + 1 - 2 * core}
    other_place = {"layer": lax.rem(layer + 2, 4)}

    w_copies = [
        pltpu.make_async_copy(wg_hbm, wg, w_sem.at[0]),
        pltpu.make_async_copy(wu_hbm, wu, w_sem.at[1]),
    ]
    for copy in w_copies:
        copy.start()

    barrier = pltpu.get_barrier_semaphore()
    for who in ({"row": right}, {"row": left}, other_col, other_core, other_place):
        pl.semaphore_signal(barrier, inc=1, device_id=who, device_id_type=MESH)
    pl.semaphore_wait(barrier, 5)

    def block_of(way, step):
        return lax.rem(row + n_row - step, n_row) if way == 0 else lax.rem(row + step, n_row)

    def ring(way, step, j):
        block = block_of(way, step - 1)
        mine = 2 * way + col
        cols = pl.ds(j * PIECE, PIECE)
        at = gath.at[block, mine, :, cols]
        return pltpu.make_async_remote_copy(
            src_ref=tok_ref.at[mine, :, cols] if step == 1 else at,
            dst_ref=at,
            send_sem=zs_sem.at[way, step - 1, j],
            recv_sem=zr_sem.at[way, step - 1, j],
            device_id={"row": right if way == 0 else left},
            device_id_type=MESH,
        )

    def across(way, step, j):
        at = gath.at[block_of(way, step), 2 * way + col, :, pl.ds(j * PIECE, PIECE)]
        return pltpu.make_async_remote_copy(
            src_ref=at,
            dst_ref=at,
            send_sem=fs_sem.at[way, step - 1, j],
            recv_sem=fr_sem.at[way, step - 1, j],
            device_id=other_col,
            device_id_type=MESH,
        )

    def place_rows(ref, block, way, first, low, high):
        rows = ref[pl.ds(2 * way, 2)].reshape(2 * quarter, depth)

        def body(i, carry):
            expert, side = lax.div(i, 2), lax.rem(i, 2)
            want = tgt_ref[block, way, expert]
            here = lax.broadcasted_iota(jnp.int32, (half, 2 * quarter), 0) + side * half
            pick = jnp.where(here == want, 1.0, 0.0).astype(jnp.bfloat16)
            got = jnp.dot(pick, rows, preferred_element_type=jnp.float32).astype(jnp.bfloat16)
            slots[expert, side] = got if first else slots[expert, side] + got
            return carry

        lax.fori_loop(2 * low, 2 * high, body, 0)

    for j in range(pieces):
        for way in range(2):
            ring(way, 1, j).start()
    place_rows(tok_ref, row, 0, True, 0, experts)
    place_rows(tok_ref, row, 1, False, 0, experts)

    def arrived(step, way):
        for j in range(pieces):
            across(way, step, j).wait_recv()

    def settle(step, way, low, high):
        block = block_of(way, step)
        place_rows(gath.at[block], block, way, False, low, high)

    for step in range(1, n_row):
        for j in range(pieces):
            for way in range(2):
                ring(way, step, j).wait_recv()
                if step + 1 < n_row:
                    ring(way, step + 1, j).start()
                across(way, step, j).start()
        if step > 1:
            for way in range(2):
                arrived(step - 1, way)
                settle(step - 1, way, 0, experts)

    for copy in w_copies:
        copy.wait()

    def core_copy(i):
        return pltpu.make_async_remote_copy(
            src_ref=dsend.at[i],
            dst_ref=drecv.at[i],
            send_sem=ds_sem.at[i],
            recv_sem=dr_sem.at[i],
            device_id=other_core,
            device_id_type=MESH,
        )

    def place_copy(i):
        return pltpu.make_async_remote_copy(
            src_ref=xsend.at[i],
            dst_ref=xrecv.at[i],
            send_sem=xs_sem.at[i],
            recv_sem=xr_sem.at[i],
            device_id=other_place,
            device_id_type=MESH,
        )

    def unit_copy(i):
        return pltpu.make_async_remote_copy(
            src_ref=unit_out.at[i],
            dst_ref=unit_in.at[i],
            send_sem=us_sem.at[i],
            recv_sem=ur_sem.at[i],
            device_id=other_place,
            device_id_type=MESH,
        )

    def col_copy(i):
        return pltpu.make_async_remote_copy(
            src_ref=ysend.at[i],
            dst_ref=yrecv.at[i],
            send_sem=ys_sem.at[i],
            recv_sem=yr_sem.at[i],
            device_id=other_col,
            device_id_type=MESH,
        )

    def multiply(i):
        expert, part = lax.div(i, per_expert), lax.rem(i, per_expert)
        cols = pl.ds(pl.multiple_of(part * CHUNK, CHUNK), CHUNK)
        for side, into in ((1 - core, dsend), (core, keep)):
            rows = slots[expert, side]
            for which, w in enumerate((wg, wu)):
                got = jnp.dot(rows, w[expert, :, cols], preferred_element_type=jnp.float32)
                into[i, which] = got.reshape(2, 2, SLOTS_DEV, CHUNK)
        core_copy(i).start()

    def pass_on(i):
        core_copy(i).wait_recv()
        away = 1 - place
        for which in range(2):
            total = keep[i, which, away] + drecv[i, which, away]
            total = total.reshape(2 * SLOTS_DEV // 8, 8, CHUNK)
            top = jnp.maximum(jnp.max(jnp.abs(total), axis=0), TINY)
            unit_out[i, which] = top * (1.0 / STEPS)
            coded = jnp.round(total * (STEPS / top)[None])
            xsend[i, which] = (
                coded.reshape(2, SLOTS_DEV, CHUNK).astype(jnp.int32).astype(jnp.int16)
            )
        unit_copy(i).start()
        place_copy(i).start()

    def first_loop(i, carry):
        multiply(i)

        @pl.when(i > 0)
        def _():
            pass_on(i - 1)

        return carry

    for expert in range(experts):
        for way in range(2):
            if expert == 0:
                arrived(n_row - 1, way)
            settle(n_row - 1, way, expert, expert + 1)
        lax.fori_loop(expert * per_expert, (expert + 1) * per_expert, first_loop, 0)
    pass_on(chunks - 1)

    def finished(i, side):
        sums = []
        for which in range(2):
            far = xrecv[i, which, side].astype(jnp.int32).astype(jnp.float32)
            far = far.reshape(SLOTS_DEV // 8, 8, CHUNK) * unit_in[i, which][None]
            near = keep[i, which, place, side] + drecv[i, which, place, side]
            sums.append(near + far.reshape(SLOTS_DEV, CHUNK))
        gate, up = sums
        return (gate / (1.0 + jnp.exp(-gate)) * up).astype(jnp.bfloat16)

    def columns(i, of_col):
        start = of_col * narrow + lax.rem(i, per_expert) * CHUNK
        return pl.ds(pl.multiple_of(start, CHUNK), CHUNK)

    def finish(i):
        unit_copy(i).wait_recv()
        place_copy(i).wait_recv()
        ysend[i] = finished(i, 1 - col)
        out_ref[lax.div(i, per_expert), :, columns(i, col)] = finished(i, col)
        col_copy(i).start()

    def take(i):
        col_copy(i).wait_recv()
        out_ref[lax.div(i, per_expert), :, columns(i, 1 - col)] = yrecv[i]

    def second_loop(i, carry):
        finish(i)

        @pl.when(i > 0)
        def _():
            take(i - 1)

        return carry

    lax.fori_loop(0, chunks, second_loop, 0)
    take(chunks - 1)

    for step in range(1, n_row):
        for way in range(2):
            for j in range(pieces):
                ring(way, step, j).wait_send()
                across(way, step, j).wait_send()

    def last_loop(i, carry):
        core_copy(i).wait_send()
        unit_copy(i).wait_send()
        place_copy(i).wait_send()
        col_copy(i).wait_send()
        return carry

    lax.fori_loop(0, chunks, last_loop, 0)


def vmem_plan(n_row, tokens, w_gate):
    local_rows, depth = tokens.shape
    experts, _, narrow = w_gate.shape
    capacity = SLOTS_DEV * 8
    chunks = experts * narrow // CHUNK
    bf, f32 = jnp.bfloat16, jnp.float32
    return [
        ((n_row, 4, local_rows // 4, depth), bf),
        (w_gate.shape, bf),
        (w_gate.shape, bf),
        ((experts, 2, capacity // 2, depth), bf),
        ((chunks, 2, 2, 2, SLOTS_DEV, CHUNK), f32),
        ((chunks, 2, 2, 2, SLOTS_DEV, CHUNK), f32),
        ((chunks, 2, 2, 2, SLOTS_DEV, CHUNK), f32),
        ((chunks, 2, 2, SLOTS_DEV, CHUNK), jnp.int16),
        ((chunks, 2, 2, SLOTS_DEV, CHUNK), jnp.int16),
        ((chunks, 2, 8, CHUNK), f32),
        ((chunks, 2, 8, CHUNK), f32),
        ((chunks, SLOTS_DEV, CHUNK), bf),
        ((chunks, SLOTS_DEV, CHUNK), bf),
    ]


def fits(n_row, n_col, n_layer, tokens, w_gate):
    local_rows, depth = tokens.shape
    narrow = w_gate.shape[2]
    if n_col != 2 or n_layer != 4 or n_row < 3:
        return False
    if local_rows % 64 or depth % PIECE or narrow % CHUNK:
        return False
    need = sum(
        functools.reduce(lambda a, b: a * b, shape) * jnp.dtype(kind).itemsize
        for shape, kind in vmem_plan(n_row, tokens, w_gate)
    )
    return need < VMEM_LIMIT - 8 * 1024 * 1024


def fused_shards(tokens, expert_ids, w_gate, w_up):
    n_row = lax.axis_size("row")
    experts, depth, narrow = w_gate.shape
    local_rows = tokens.shape[0]
    quarter = local_rows // 4
    chunks = experts * narrow // CHUNK
    pieces = depth // PIECE
    member, rank = slot_places(expert_ids, experts)
    of_col, of_layer, inner = rank // (4 * SLOTS_DEV), rank // SLOTS_DEV % 4, rank % SLOTS_DEV
    spot = ((of_layer % 2 * 2 + of_layer // 2) * 2 + of_col) * SLOTS_DEV + inner
    target = jnp.where(member > 0, spot, -1)
    target = target.reshape(n_row, 2, 1, 2 * quarter, experts).transpose(0, 1, 4, 2, 3)
    dma = pltpu.SemaphoreType.DMA
    ring_sems = dma((2, n_row - 1, pieces))
    return pl.pallas_call(
        functools.partial(kernel, n_row),
        out_shape=jax.ShapeDtypeStruct((experts, SLOTS_DEV, 2 * narrow), jnp.bfloat16),
        in_specs=[
            pl.BlockSpec(memory_space=pltpu.VMEM),
            pl.BlockSpec(memory_space=pltpu.VMEM),
            pl.BlockSpec(memory_space=pl.ANY),
            pl.BlockSpec(memory_space=pl.ANY),
        ],
        out_specs=pl.BlockSpec(memory_space=pltpu.VMEM),
        scratch_shapes=[
            pltpu.VMEM(shape, kind) for shape, kind in vmem_plan(n_row, tokens, w_gate)
        ]
        + [dma((2,))]
        + [ring_sems] * 4
        + [dma((chunks,))] * 8,
        compiler_params=pltpu.CompilerParams(
            collective_id=0, has_side_effects=True, vmem_limit_bytes=VMEM_LIMIT
        ),
    )(tokens.reshape(4, quarter, depth), target, w_gate, w_up)


def solution(mesh):
    def shards(tokens, expert_ids, w_gate, w_up):
        sizes = [mesh.shape[axis] for axis in ("row", "col", "layer")]
        plan = fused_shards if fits(*sizes, tokens, w_gate) else plain_shards
        return plan(tokens, expert_ids, w_gate, w_up)

    in_specs = (
        P("row", "layer"),
        P(),
        P(None, "layer", ("row", "col")),
        P(None, "layer", ("row", "col")),
    )
    out_specs = P(None, ("col", "layer"), "row")
    return jax.shard_map(shards, mesh=mesh, in_specs=in_specs, out_specs=out_specs, check_vma=False)
```
